128 devices in a mesh: row: 4 (over z), col: 32 (over y, x, core).
Axes of the slice: x: 4, y: 4, z: 4, core: 2. Of those that a mesh axis runs over, the one named last changes fastest.
Arguments:
- eigvecs: float32 [16384, 8192], P('row', 'col'), may hold values from -6 to 6
- v_panels: float32 [8, 16384, 256], P(None, 'row', 'col'), as said below
- t_panels: float32 [8, 256, 256], P(None, None, 'col'), as said below
Outputs:
- rotated: float32 [16384, 8192], P('row', 'col')
The draws below stay inside these ranges and needn't reach their ends.
Inputs may be any that keep to these rules, and one draw needn't show every extreme that they name: `v_panels`: in panel k, vector j is zero in rows above k * 256 + j + 1, equals 1 in that row and is dense below it. t_panels[k] is upper triangular and V_k t_panels[k] V_k^T = I minus the product of the panel's 256 Householder reflections, each I - 2 v v^T / (v^T v), taken in the order of j; its diagonal lies in (0, 2].
All inputs are finite; a program needn't handle non-finite values.
Results may differ from the reference program's by a relative error of at most 0.00015.
Values sent between devices are 32-bit elements; how exact they have to be, the bound alone decides.
A program may use at most 128 MiB of HBM per device.

```python
import math
import jax
import jax.numpy as jnp
from jax import lax

ORDER = 16384
PANEL_W = 256
PANELS = 8
COLS = 8192


def householder_panels(key):
    noise = jax.random.normal(jax.random.fold_in(key, 7), (PANELS, ORDER, PANEL_W), jnp.float32) / math.sqrt(ORDER)
    rows_at = lax.broadcasted_iota(jnp.int32, (PANELS, ORDER, PANEL_W), 1)
    column_at = lax.broadcasted_iota(jnp.int32, (PANELS, ORDER, PANEL_W), 2)
    panel_at = lax.broadcasted_iota(jnp.int32, (PANELS, ORDER, PANEL_W), 0)
    unit_row = panel_at * PANEL_W + column_at + 1
    return jnp.where(rows_at > unit_row, noise, jnp.where(rows_at == unit_row, 1.0, 0.0)).astype(jnp.float32)


def draw_v_panels(key, part):
    return householder_panels(key)


def draw_t_panels(key, part):
    vectors = householder_panels(key)
    gram = jnp.einsum('knb,knc->kbc', vectors, vectors, precision=lax.Precision.HIGHEST)
    identity = jnp.eye(PANEL_W, dtype=jnp.float32)
    inverse_factor = jnp.triu(gram, 1) + 0.5 * gram * identity
    eye_stack = jnp.broadcast_to(identity, (PANELS, PANEL_W, PANEL_W))
    factor = lax.linalg.triangular_solve(inverse_factor, eye_stack, left_side=True, lower=False)
    return jnp.triu(factor).astype(jnp.float32)


def block_scale(own_key, shape, split, least, largest):
    level = 1.0
    for position, shards_of in split:
        draws = jax.random.uniform(jax.random.fold_in(jax.random.fold_in(own_key, 6), position), (shards_of,), jnp.float32, least / len(split), largest / len(split))
        level = level * jnp.repeat(jnp.exp(draws), shape[position] // shards_of).reshape((-1,) + (1,) * (len(shape) - 1 - position))
    return level


def scatter_about(rng, shape, deviation, most, pieces=(), held_as=jnp.bfloat16):
    loudness = block_scale(rng, shape, pieces, -0.22, 0.18) if pieces else 1.0
    drawn = jax.random.normal(rng, shape, jnp.float32) * deviation * loudness
    return jnp.minimum(jnp.maximum(drawn, -most), most).astype(held_as)


def setup_inputs(seed: int = 0) -> dict:
    keys = jax.random.split(jax.random.key(seed), 4)
    return {
        "eigvecs": scatter_about(keys[0], (ORDER, COLS), 1.0, 6.0, ((0, 4), (1, 32)), jnp.float32),
        "v_panels": draw_v_panels(jax.random.fold_in(keys[3], 71), 0),
        "t_panels": draw_t_panels(jax.random.fold_in(keys[3], 71), 0),
    }


def reference(eigvecs, v_panels, t_panels):
    current = eigvecs
    for panel_index in reversed(range(PANELS)):
        vectors = v_panels[panel_index]
        projected = jnp.dot(vectors.T.astype(jnp.float32), current.astype(jnp.float32), preferred_element_type=jnp.float32, precision=lax.Precision.HIGHEST)
        scaled = jnp.dot(t_panels[panel_index].astype(jnp.float32), projected.astype(jnp.float32), preferred_element_type=jnp.float32, precision=lax.Precision.HIGHEST)
        current = current - jnp.dot(vectors.astype(jnp.float32), scaled.astype(jnp.float32), preferred_element_type=jnp.float32, precision=lax.Precision.HIGHEST)
    return current
```

```python
import jax
import jax.numpy as jnp
from jax import lax
from jax.experimental import pallas as pl
from jax.experimental.pallas import tpu as pltpu
from jax.sharding import PartitionSpec as P

MESH = pl.DeviceIdType.MESH
F32, BF16 = jnp.float32, jnp.bfloat16
PANELS, WIDTH, ROWS, COLS = 8, 256, 4096, 256
SIDE, STRIPE = 4, 8
LANES = ROWS + WIDTH
CHUNK = 1024
SPANS = ((0, 1024), (1024, 1024), (2048, 1024), (3072, 1280))
QUARTERS = len(SPANS)
BLOCK = 512
AHEAD = 2


def halves(x):
    high = x.astype(BF16)
    return high, (x - high.astype(F32)).astype(BF16)


def dot3(left, right):
    (lh, ll), (rh, rl) = left, right
    dot = lambda u, v: jnp.dot(u, v, preferred_element_type=F32)
    return dot(lh, rh) + dot(lh, rl) + dot(ll, rh)


def kernel(
    z_in, v_in, t_in, z_out,
    vbuf, z, zh, zl, vh, vl, vnh, vnl, proj, gram, psend, prec, sfull, sh, sl,
    load_sem, z_sem, out_sem,
    near_sem, half_sem, row_sem, rowhalf_sem, core_sem, sent1, sent2, sent3,
    rs_sem, rs_sent, ag_sem, ag_sent,
):
    row, col = lax.axis_index("row"), lax.axis_index("col")
    core, x, y = lax.rem(col, 2), lax.rem(col // 2, SIDE), col // (2 * SIDE)
    a, b = x + core * (y - x), y + core * (x - y)
    step_a, step_b = 1 + 3 * core, 4 - 3 * core
    wrap = lambda i: lax.rem(i + SIDE, SIDE)

    def at(a_to, b_to):
        return (row, 2 * (a_to * step_a + b_to * step_b) + core)

    a_next, a_prev, b_next, b_prev = wrap(a + 1), wrap(a - 1), wrap(b + 1), wrap(b - 1)
    a_far, b_far = wrap(a + 2), wrap(b + 2)
    up_a, down_a, up_b, down_b = at(a_next, b), at(a_prev, b), at(a, b_next), at(a, b_prev)
    partner = (row, col + 1 - 2 * core)
    lifts = [(wrap(row + d), col) for d in (1, 2, 3)]

    def copy(src, dst, send, recv, device):
        return pltpu.make_async_remote_copy(
            src_ref=src, dst_ref=dst, send_sem=send, recv_sem=recv, device_id=device, device_id_type=MESH
        )

    def push(ref, send, recv, device):
        copy(ref, ref, send, recv, device).start()

    def arrived(ref, recv):
        copy(ref, ref, sent1.at[0], recv, partner).wait_recv()

    def gone(ref, send):
        copy(ref, ref, send, core_sem.at[0, 0], partner).wait_send()

    def stripe(n, q, a_of, part=None):
        start, size = SPANS[q]
        if part is not None:
            size //= 2
            start += part * size
        return vbuf.at[n, core, b, a_of, :, pl.ds(start, size)]

    def line(n, q, b_of, part=None):
        start, size = SPANS[q]
        first, count = (0, SIDE) if part is None else (2 * part, 2)
        return vbuf.at[n, core, b_of, pl.ds(first, count), :, pl.ds(start, size)]

    def load(n):
        own = lambda start, size: vbuf.at[n, core, b, a, :, pl.ds(start, size)]
        return (
            pltpu.make_async_copy(v_in.at[PANELS - 1 - n], own(0, ROWS), load_sem.at[n, 0]),
            pltpu.make_async_copy(t_in.at[PANELS - 1 - n], own(ROWS, WIDTH), load_sem.at[n, 1]),
        )

    def wait_load(n):
        for one in load(n):
            one.wait()

    def first_send(n, q):
        push(stripe(n, q, a), sent1.at[n], near_sem.at[n, q, 0], up_a)
        push(stripe(n, q, a), sent1.at[n], near_sem.at[n, q, 1], down_a)

    def stage_a(n, q):
        arrived(stripe(n, q, a_prev), near_sem.at[n, q, 0])
        push(stripe(n, q, a_prev, 0), sent1.at[n], half_sem.at[n, q, 0], up_a)
        arrived(stripe(n, q, a_next), near_sem.at[n, q, 1])
        push(stripe(n, q, a_next, 1), sent1.at[n], half_sem.at[n, q, 1], down_a)

    def stage_b(n, q):
        arrived(stripe(n, q, a_far, 0), half_sem.at[n, q, 0])
        arrived(stripe(n, q, a_far, 1), half_sem.at[n, q, 1])
        push(line(n, q, b), sent2.at[n], row_sem.at[n, q, 0], up_b)
        push(line(n, q, b), sent2.at[n], row_sem.at[n, q, 1], down_b)
        push(line(n, q, b), sent3.at[n], core_sem.at[n, q], partner)

    def stage_c(n, q):
        arrived(line(n, q, b_prev), row_sem.at[n, q, 0])
        push(line(n, q, b_prev, 0), sent2.at[n], rowhalf_sem.at[n, q, 0], up_b)
        push(line(n, q, b_prev), sent3.at[n], core_sem.at[n, q], partner)
        arrived(line(n, q, b_next), row_sem.at[n, q, 1])
        push(line(n, q, b_next, 1), sent2.at[n], rowhalf_sem.at[n, q, 1], down_b)
        push(line(n, q, b_next), sent3.at[n], core_sem.at[n, q], partner)

    def stage_d(n, q):
        arrived(line(n, q, b_far, 0), rowhalf_sem.at[n, q, 0])
        arrived(line(n, q, b_far, 1), rowhalf_sem.at[n, q, 1])
        push(line(n, q, b_far), sent3.at[n], core_sem.at[n, q], partner)

    def stage_e(n, q):
        start, size = SPANS[q]
        arrived(vbuf.at[n, 1 - core, :, :, :, pl.ds(start, size)], core_sem.at[n, q])

    def pair(n, i, start, size):
        yy, xx = divmod(i, SIDE)
        lanes = pl.ds(start, size)
        return jnp.concatenate([vbuf[n, 0, yy, xx, :, lanes], vbuf[n, 1, xx, yy, :, lanes]], axis=0)

    def absorb(n, q):
        slot = lax.rem(n, 2)
        rows = pl.ds(CHUNK * q, CHUNK)
        for i in range(SIDE * SIDE):
            high, low = halves(pair(n, i, CHUNK * q, CHUNK))
            vh[pl.ds(2 * STRIPE * i, 2 * STRIPE), :] = high
            vl[pl.ds(2 * STRIPE * i, 2 * STRIPE), :] = low
        vnh[slot, rows, :] = vh[...].T
        vnl[slot, rows, :] = vl[...].T
        left = (vh[...], vl[...])
        part = dot3(left, (zh[rows, :], zl[rows, :]))
        proj[...] = part if q == 0 else proj[...] + part

        @pl.when(n > 0)
        def _():
            part = dot3(left, (vnh[1 - slot, rows, :], vnl[1 - slot, rows, :]))
            gram[...] = part if q == 0 else gram[...] + part

    quarter = COLS // 4
    own_rows = pl.ds(pl.multiple_of(quarter * row, quarter), quarter)

    def take_s(n):
        for d in (1, 2, 3):
            rows = pl.ds(pl.multiple_of(quarter * wrap(row - d), quarter), quarter)
            arrived(sfull.at[n, rows], ag_sem.at[n, d - 1])
        sh[...], sl[...] = halves(sfull[n].T)

    def finish(n):
        @pl.when(n > 0)
        def _():
            take_s(n - 1)
            proj[...] = proj[...] - dot3(halves(gram[...]), (sh[...], sl[...]))

        psend[n] = proj[...].T
        for d in (1, 2, 3):
            rows = pl.ds(pl.multiple_of(quarter * wrap(row + d), quarter), quarter)
            copy(psend.at[n, rows], prec.at[n, d - 1], rs_sent.at[n], rs_sem.at[n, d - 1], lifts[d - 1]).start()

    def scale(n):
        total = psend[n, own_rows, :]
        for d in (1, 2, 3):
            arrived(prec.at[n, d - 1], rs_sem.at[n, d - 1])
        for d in (1, 2, 3):
            total = total + prec[n, d - 1]
        factor = jnp.concatenate([pair(n, i, ROWS, WIDTH) for i in range(SIDE * SIDE)], axis=0)
        sfull[n, own_rows, :] = dot3(halves(total), halves(factor))
        for d in (1, 2, 3):
            push(sfull.at[n, own_rows], ag_sent.at[n], ag_sem.at[n, d - 1], lifts[d - 1])

    def write(i):
        rows = pl.ds(pl.multiple_of(i * BLOCK, BLOCK), BLOCK)
        return pltpu.make_async_copy(z.at[rows], z_out.at[rows], out_sem.at[i])

    def update(n, last=False):
        slot = lax.rem(n, 2)

        def body(i, carry):
            rows = pl.ds(pl.multiple_of(i * BLOCK, BLOCK), BLOCK)
            new = z[rows, :] - dot3((vnh[slot, rows, :], vnl[slot, rows, :]), (sh[...], sl[...]))
            z[rows, :] = new
            if last:
                write(i).start()
            else:
                zh[rows, :], zl[rows, :] = halves(new)
            return carry

        lax.fori_loop(0, ROWS // BLOCK, body, 0)

    z_load = pltpu.make_async_copy(z_in, z, z_sem)

    def start_load(n, carry):
        for one in load(n):
            one.start()
        return carry

    lax.fori_loop(0, PANELS, start_load, 0)
    z_load.start()

    barrier = pltpu.get_barrier_semaphore()
    greeted = [up_a, down_a, up_b, down_b, partner] + lifts
    for device in greeted:
        pl.semaphore_signal(barrier, inc=1, device_id=device, device_id_type=MESH)
    pl.semaphore_wait(barrier, len(greeted))

    def open_sends(n, carry):
        wait_load(n)
        for q in range(QUARTERS):
            first_send(n, q)
        return carry

    lax.fori_loop(0, AHEAD, open_sends, 0)
    z_load.wait()

    def split_z(i, carry):
        rows = pl.ds(pl.multiple_of(i * BLOCK, BLOCK), BLOCK)
        zh[rows, :], zl[rows, :] = halves(z[rows, :])
        return carry

    lax.fori_loop(0, ROWS // BLOCK, split_z, 0)

    def panel(p, carry):
        for q in range(QUARTERS):

            @pl.when(p + AHEAD < PANELS)
            def _():
                if q == 0:
                    wait_load(p + AHEAD)
                first_send(p + AHEAD, q)

            for back, stage in ((0, stage_a), (1, stage_b), (2, stage_c), (3, stage_d)):
                behind, at_q = (0, q - back) if q >= back else (1, q - back + QUARTERS)
                when = (p < PANELS) if behind == 0 else (p > 0)
                pl.when(when)(lambda: stage(p - behind, at_q))

            n = p - 1

            @pl.when(p > 0)
            def _():
                stage_e(n, q)
                if q == 0:
                    pl.when(n > 1)(lambda: update(n - 2))
                absorb(n, q)
                if q == 1:
                    pl.when(n > 0)(lambda: scale(n - 1))
                if q == QUARTERS - 1:
                    finish(n)

        return carry

    lax.fori_loop(0, PANELS + 1, panel, 0)

    update(PANELS - 2)
    scale(PANELS - 1)
    take_s(PANELS - 1)
    update(PANELS - 1, last=True)

    def close(n, carry):
        gone(vbuf.at[n, 0, 0, pl.ds(0, 3)], sent1.at[n])
        gone(vbuf.at[n, 0, pl.ds(0, 3)], sent2.at[n])
        gone(vbuf.at[n, 0], sent3.at[n])
        gone(prec.at[n], rs_sent.at[n])
        gone(prec.at[n], ag_sent.at[n])
        return carry

    lax.fori_loop(0, PANELS, close, 0)

    def close_out(i, carry):
        write(i).wait()
        return carry

    lax.fori_loop(0, ROWS // BLOCK, close_out, 0)


def local(eigvecs, v_panels, t_panels):
    dma = pltpu.SemaphoreType.DMA
    anywhere = pl.BlockSpec(memory_space=pl.ANY)
    return pl.pallas_call(
        kernel,
        out_shape=jax.ShapeDtypeStruct((ROWS, COLS), F32),
        in_specs=[anywhere] * 3,
        out_specs=anywhere,
        scratch_shapes=[
            pltpu.VMEM((PANELS, 2, SIDE, SIDE, STRIPE, LANES), F32),
            pltpu.VMEM((ROWS, COLS), F32),
            pltpu.VMEM((ROWS, COLS), BF16),
            pltpu.VMEM((ROWS, COLS), BF16),
            pltpu.VMEM((WIDTH, CHUNK), BF16),
            pltpu.VMEM((WIDTH, CHUNK), BF16),
            pltpu.VMEM((2, ROWS, WIDTH), BF16),
            pltpu.VMEM((2, ROWS, WIDTH), BF16),
            pltpu.VMEM((WIDTH, COLS), F32),
            pltpu.VMEM((WIDTH, WIDTH), F32),
            pltpu.VMEM((PANELS, COLS, WIDTH), F32),
            pltpu.VMEM((PANELS, 3, COLS // 4, WIDTH), F32),
            pltpu.VMEM((PANELS, COLS, WIDTH), F32),
            pltpu.VMEM((WIDTH, COLS), BF16),
            pltpu.VMEM((WIDTH, COLS), BF16),
            dma((PANELS, 2)),
            dma,
            dma((ROWS // BLOCK,)),
            dma((PANELS, QUARTERS, 2)),
            dma((PANELS, QUARTERS, 2)),
            dma((PANELS, QUARTERS, 2)),
            dma((PANELS, QUARTERS, 2)),
            dma((PANELS, QUARTERS)),
            dma((PANELS,)),
            dma((PANELS,)),
            dma((PANELS,)),
            dma((PANELS, 3)),
            dma((PANELS,)),
            dma((PANELS, 3)),
            dma((PANELS,)),
        ],
        compiler_params=pltpu.CompilerParams(
            collective_id=0, has_side_effects=True, vmem_limit_bytes=67043328
        ),
    )(eigvecs, jnp.swapaxes(v_panels, 1, 2), jnp.swapaxes(t_panels, 1, 2))


def solution(mesh):
    in_specs = (P("row", "col"), P(None, "row", "col"), P(None, None, "col"))
    out_specs = P("row", "col")
    return jax.shard_map(local, mesh=mesh, in_specs=in_specs, out_specs=out_specs, check_vma=False)
```

```python
import jax
import jax.numpy as jnp
from jax import lax
from jax.experimental import pallas as pl
from jax.experimental.pallas import tpu as pltpu
from jax.sharding import PartitionSpec as P

MESH = pl.DeviceIdType.MESH
F32, BF16 = jnp.float32, jnp.bfloat16
PANELS, WIDTH, ROWS, COLS = 8, 256, 4096, 256
SIDE, STRIPE = 4, 8
LANES = ROWS + WIDTH
CHUNK = 1024
SPANS = ((0, 1024), (1024, 1024), (2048, 1024), (3072, 1280))
QUARTERS = len(SPANS)
BLOCK = 512
AHEAD = 2
LAGS = (0, 2, 4, 6, 8)


def halves(x):
    high = x.astype(BF16)
    return high, (x - high.astype(F32)).astype(BF16)


def dot3(left, right):
    (lh, ll), (rh, rl) = left, right
    dot = lambda u, v: jnp.dot(u, v, preferred_element_type=F32)
    return dot(lh, rh) + dot(lh, rl) + dot(ll, rh)


def kernel(
    z_in, v_in, t_in, z,
    vbuf, zh, zl, vh, vl, vnh, vnl, both, psend, prec, sfull, sh, sl,
    load_sem, z_sem,
    near_sem, half_sem, row_sem, rowhalf_sem, core_sem, sent1, sent2, sent3,
    rs_sem, rs_sent, ag_sem, ag_sent,
):
    row, col = lax.axis_index("row"), lax.axis_index("col")
    core, x, y = lax.rem(col, 2), lax.rem(col // 2, SIDE), col // (2 * SIDE)
    a, b = x + core * (y - x), y + core * (x - y)
    step_a, step_b = 1 + 3 * core, 4 - 3 * core
    wrap = lambda i: lax.rem(i + SIDE, SIDE)

    def at(a_to, b_to):
        return (row, 2 * (a_to * step_a + b_to * step_b) + core)

    a_next, a_prev, b_next, b_prev = wrap(a + 1), wrap(a - 1), wrap(b + 1), wrap(b - 1)
    a_far, b_far = wrap(a + 2), wrap(b + 2)
    up_a, down_a, up_b, down_b = at(a_next, b), at(a_prev, b), at(a, b_next), at(a, b_prev)
    partner = (row, col + 1 - 2 * core)
    lifts = [(wrap(row + d), col) for d in (1, 2, 3)]

    def copy(src, dst, send, recv, device):
        return pltpu.make_async_remote_copy(
            src_ref=src, dst_ref=dst, send_sem=send, recv_sem=recv, device_id=device, device_id_type=MESH
        )

    def push(ref, send, recv, device):
        copy(ref, ref, send, recv, device).start()

    def arrived(ref, recv):
        copy(ref, ref, sent1.at[0], recv, partner).wait_recv()

    def gone(ref, send):
        copy(ref, ref, send, core_sem.at[0, 0], partner).wait_send()

    def stripe(n, q, a_of, part=None):
        start, size = SPANS[q]
        if part is not None:
            size //= 2
            start += part * size
        return vbuf.at[n, core, b, a_of, :, pl.ds(start, size)]

    def line(n, q, b_of, part=None):
        start, size = SPANS[q]
        first, count = (0, SIDE) if part is None else (2 * part, 2)
        return vbuf.at[n, core, b_of, pl.ds(first, count), :, pl.ds(start, size)]

    def load(n):
        own = lambda start, size: vbuf.at[n, core, b, a, :, pl.ds(start, size)]
        return (
            pltpu.make_async_copy(v_in.at[PANELS - 1 - n], own(0, ROWS), load_sem.at[n, 0]),
            pltpu.make_async_copy(t_in.at[PANELS - 1 - n], own(ROWS, WIDTH), load_sem.at[n, 1]),
        )

    def wait_load(n):
        for one in load(n):
            one.wait()

    def first_send(n, q):
        push(stripe(n, q, a), sent1.at[n], near_sem.at[n, q, 0], up_a)
        push(stripe(n, q, a), sent1.at[n], near_sem.at[n, q, 1], down_a)

    def stage_a(n, q):
        arrived(stripe(n, q, a_prev), near_sem.at[n, q, 0])
        push(stripe(n, q, a_prev, 0), sent1.at[n], half_sem.at[n, q, 0], up_a)
        arrived(stripe(n, q, a_next), near_sem.at[n, q, 1])
        push(stripe(n, q, a_next, 1), sent1.at[n], half_sem.at[n, q, 1], down_a)

    def stage_b(n, q):
        arrived(stripe(n, q, a_far, 0), half_sem.at[n, q, 0])
        arrived(stripe(n, q, a_far, 1), half_sem.at[n, q, 1])
        push(line(n, q, b), sent2.at[n], row_sem.at[n, q, 0], up_b)
        push(line(n, q, b), sent2.at[n], row_sem.at[n, q, 1], down_b)
        push(line(n, q, b), sent3.at[n], core_sem.at[n, q], partner)

    def stage_c(n, q):
        arrived(line(n, q, b_prev), row_sem.at[n, q, 0])
        push(line(n, q, b_prev, 0), sent2.at[n], rowhalf_sem.at[n, q, 0], up_b)
        push(line(n, q, b_prev), sent3.at[n], core_sem.at[n, q], partner)
        arrived(line(n, q, b_next), row_sem.at[n, q, 1])
        push(line(n, q, b_next, 1), sent2.at[n], rowhalf_sem.at[n, q, 1], down_b)
        push(line(n, q, b_next), sent3.at[n], core_sem.at[n, q], partner)

    def stage_d(n, q):
        arrived(line(n, q, b_far, 0), rowhalf_sem.at[n, q, 0])
        arrived(line(n, q, b_far, 1), rowhalf_sem.at[n, q, 1])
        push(line(n, q, b_far), sent3.at[n], core_sem.at[n, q], partner)

    def stage_e(n, q):
        start, size = SPANS[q]
        arrived(vbuf.at[n, 1 - core, :, :, :, pl.ds(start, size)], core_sem.at[n, q])

    def pair(n, i, start, size):
        yy, xx = divmod(i, SIDE)
        lanes = pl.ds(start, size)
        return jnp.concatenate([vbuf[n, 0, yy, xx, :, lanes], vbuf[n, 1, xx, yy, :, lanes]], axis=0)

    def absorb(n, q):
        slot = lax.rem(n, 2)
        rows = pl.ds(CHUNK * q, CHUNK)
        for i in range(SIDE * SIDE):
            high, low = halves(pair(n, i, CHUNK * q, CHUNK))
            vh[pl.ds(2 * STRIPE * i, 2 * STRIPE), :] = high
            vl[pl.ds(2 * STRIPE * i, 2 * STRIPE), :] = low
        vnh[slot, rows, :] = vh[...].T
        vnl[slot, rows, :] = vl[...].T
        right = (
            jnp.concatenate([zh[rows, :], vnh[1 - slot, rows, :]], axis=1),
            jnp.concatenate([zl[rows, :], vnl[1 - slot, rows, :]], axis=1),
        )
        part = dot3((vh[...], vl[...]), right)
        both[...] = part if q == 0 else both[...] + part

    quarter = COLS // 4
    own_rows = pl.ds(pl.multiple_of(quarter * row, quarter), quarter)

    def take_s(n):
        for d in (1, 2, 3):
            rows = pl.ds(pl.multiple_of(quarter * wrap(row - d), quarter), quarter)
            arrived(sfull.at[n, rows], ag_sem.at[n, d - 1])
        sh[...], sl[...] = halves(sfull[n].T)

    def finish(n):
        @pl.when(n == 0)
        def _():
            psend[n] = both[:, :COLS].T

        @pl.when(n > 0)
        def _():
            take_s(n - 1)
            psend[n] = (both[:, :COLS] - dot3(halves(both[:, COLS:]), (sh[...], sl[...]))).T

        for d in (1, 2, 3):
            rows = pl.ds(pl.multiple_of(quarter * wrap(row + d), quarter), quarter)
            copy(psend.at[n, rows], prec.at[n, d - 1], rs_sent.at[n], rs_sem.at[n, d - 1], lifts[d - 1]).start()

    def scale(n):
        total = psend[n, own_rows, :]
        for d in (1, 2, 3):
            arrived(prec.at[n, d - 1], rs_sem.at[n, d - 1])
        for d in (1, 2, 3):
            total = total + prec[n, d - 1]
        factor = jnp.concatenate([pair(n, i, ROWS, WIDTH) for i in range(SIDE * SIDE)], axis=0)
        sfull[n, own_rows, :] = dot3(halves(total), halves(factor))
        for d in (1, 2, 3):
            push(sfull.at[n, own_rows], ag_sent.at[n], ag_sem.at[n, d - 1], lifts[d - 1])

    def update_rows(n, q):
        slot, rows = lax.rem(n, 2), pl.ds(CHUNK * q, CHUNK)
        new = z[rows, :] - dot3((vnh[slot, rows, :], vnl[slot, rows, :]), (sh[...], sl[...]))
        z[rows, :] = new
        zh[rows, :], zl[rows, :] = halves(new)

    def update(n, last=False):
        slot = lax.rem(n, 2)

        def body(i, carry):
            rows = pl.ds(pl.multiple_of(i * BLOCK, BLOCK), BLOCK)
            new = z[rows, :] - dot3((vnh[slot, rows, :], vnl[slot, rows, :]), (sh[...], sl[...]))
            z[rows, :] = new
            if not last:
                zh[rows, :], zl[rows, :] = halves(new)
            return carry

        lax.fori_loop(0, ROWS // BLOCK, body, 0)

    z_load = pltpu.make_async_copy(z_in, z, z_sem)

    def start_load(n, carry):
        for one in load(n):
            one.start()
        return carry

    lax.fori_loop(0, PANELS, start_load, 0)
    z_load.start()

    barrier = pltpu.get_barrier_semaphore()
    greeted = [up_a, down_a, up_b, down_b, partner] + lifts
    for device in greeted:
        pl.semaphore_signal(barrier, inc=1, device_id=device, device_id_type=MESH)
    pl.semaphore_wait(barrier, len(greeted))

    def open_sends(n, carry):
        wait_load(n)
        for q in range(QUARTERS):
            first_send(n, q)
        return carry

    lax.fori_loop(0, AHEAD, open_sends, 0)
    z_load.wait()

    def split_z(i, carry):
        rows = pl.ds(pl.multiple_of(i * BLOCK, BLOCK), BLOCK)
        zh[rows, :], zl[rows, :] = halves(z[rows, :])
        return carry

    lax.fori_loop(0, ROWS // BLOCK, split_z, 0)

    def panel(p, carry):
        def behind(q, lag):
            return p + (q - lag) // QUARTERS, (q - lag) % QUARTERS

        for q in range(QUARTERS):

            @pl.when(p + AHEAD < PANELS)
            def _():
                if q == 0:
                    wait_load(p + AHEAD)
                first_send(p + AHEAD, q)

            for lag, stage in zip(LAGS, (stage_a, stage_b, stage_c, stage_d)):
                m, at_q = behind(q, lag)
                pl.when((m >= 0) & (m < PANELS))(lambda: stage(m, at_q))

            n, at_q = behind(q, LAGS[-1])

            @pl.when((n >= 0) & (n < PANELS))
            def _():
                stage_e(n, at_q)
                pl.when(n > 1)(lambda: update_rows(n - 2, at_q))
                absorb(n, at_q)
                if at_q == 1:
                    pl.when(n > 0)(lambda: scale(n - 1))
                if at_q == QUARTERS - 1:
                    finish(n)

        return carry

    lax.fori_loop(0, PANELS + -(-LAGS[-1] // QUARTERS), panel, 0)

    update(PANELS - 2)
    scale(PANELS - 1)
    take_s(PANELS - 1)
    update(PANELS - 1, last=True)

    def close(n, carry):
        gone(vbuf.at[n, 0, 0, pl.ds(0, 3)], sent1.at[n])
        gone(vbuf.at[n, 0, pl.ds(0, 3)], sent2.at[n])
        gone(vbuf.at[n, 0], sent3.at[n])
        gone(prec.at[n], rs_sent.at[n])
        gone(prec.at[n], ag_sent.at[n])
        return carry

    lax.fori_loop(0, PANELS, close, 0)


def local(eigvecs, v_panels, t_panels):
    dma = pltpu.SemaphoreType.DMA
    anywhere = pl.BlockSpec(memory_space=pl.ANY)
    return pl.pallas_call(
        kernel,
        out_shape=pltpu.VMEM((ROWS, COLS), F32),
        in_specs=[anywhere] * 3,
        out_specs=pl.BlockSpec(memory_space=pltpu.VMEM),
        scratch_shapes=[
            pltpu.VMEM((PANELS, 2, SIDE, SIDE, STRIPE, LANES), F32),
            pltpu.VMEM((ROWS, COLS), BF16),
            pltpu.VMEM((ROWS, COLS), BF16),
            pltpu.VMEM((WIDTH, CHUNK), BF16),
            pltpu.VMEM((WIDTH, CHUNK), BF16),
            pltpu.VMEM((2, ROWS, WIDTH), BF16),
            pltpu.VMEM((2, ROWS, WIDTH), BF16),
            pltpu.VMEM((WIDTH, COLS + WIDTH), F32),
            pltpu.VMEM((PANELS, COLS, WIDTH), F32),
            pltpu.VMEM((PANELS, 3, COLS // 4, WIDTH), F32),
            pltpu.VMEM((PANELS, COLS, WIDTH), F32),
            pltpu.VMEM((WIDTH, COLS), BF16),
            pltpu.VMEM((WIDTH, COLS), BF16),
            dma((PANELS, 2)),
            dma,
            dma((PANELS, QUARTERS, 2)),
            dma((PANELS, QUARTERS, 2)),
            dma((PANELS, QUARTERS, 2)),
            dma((PANELS, QUARTERS, 2)),
            dma((PANELS, QUARTERS)),
            dma((PANELS,)),
            dma((PANELS,)),
            dma((PANELS,)),
            dma((PANELS, 3)),
            dma((PANELS,)),
            dma((PANELS, 3)),
            dma((PANELS,)),
        ],
        compiler_params=pltpu.CompilerParams(
            collective_id=0, has_side_effects=True, vmem_limit_bytes=58 * 2**20
        ),
    )(eigvecs, jnp.swapaxes(v_panels, 1, 2), jnp.swapaxes(t_panels, 1, 2))


def solution(mesh):
    in_specs = (P("row", "col"), P(None, "row", "col"), P(None, None, "col"))
    out_specs = P("row", "col")
    return jax.shard_map(local, mesh=mesh, in_specs=in_specs, out_specs=out_specs, check_vma=False)
```

```python
import jax
import jax.numpy as jnp
from jax import lax
from jax.experimental import pallas as pl
from jax.experimental.pallas import tpu as pltpu
from jax.sharding import PartitionSpec as P

MESH = pl.DeviceIdType.MESH
F32, BF16 = jnp.float32, jnp.bfloat16
PANELS, WIDTH, ROWS, COLS = 8, 256, 4096, 256
SIDE, STRIPE = 4, 8
LANES = ROWS + WIDTH
CHUNK = 1024
SPANS = ((0, 1024), (1024, 1024), (2048, 1024), (3072, 1280))
QUARTERS = len(SPANS)
BLOCK = 1024
AHEAD = 3
EARLY = 1
LAGS = (0, 2, 4, 6, 7)


def halves(x):
    high = x.astype(BF16)
    return high, (x - high.astype(F32)).astype(BF16)


def dot3(left, right):
    (lh, ll), (rh, rl) = left, right
    dot = lambda u, v: jnp.dot(u, v, preferred_element_type=F32)
    return dot(lh, rh) + dot(lh, rl) + dot(ll, rh)


def kernel(
    z_in, v_in, t_in, z,
    vbuf, zh, zl, vh, vl, vnh, vnl, both, psend, prec, sfull, sh, sl, th, tl,
    load_sem, z_sem,
    near_sem, half_sem, row_sem, rowhalf_sem, core_sem, sent1, sent2, sent3,
    rs_sem, rs_sent, ag_sem, ag_sent,
):
    row, col = lax.axis_index("row"), lax.axis_index("col")
    core, x, y = lax.rem(col, 2), lax.rem(col // 2, SIDE), col // (2 * SIDE)
    a, b = x + core * (y - x), y + core * (x - y)
    step_a, step_b = 1 + 3 * core, 4 - 3 * core
    wrap = lambda i: lax.rem(i + SIDE, SIDE)

    def at(a_to, b_to):
        return (row, 2 * (a_to * step_a + b_to * step_b) + core)

    a_next, a_prev, b_next, b_prev = wrap(a + 1), wrap(a - 1), wrap(b + 1), wrap(b - 1)
    a_far, b_far = wrap(a + 2), wrap(b + 2)
    up_a, down_a, up_b, down_b = at(a_next, b), at(a_prev, b), at(a, b_next), at(a, b_prev)
    partner = (row, col + 1 - 2 * core)
    lifts = [(wrap(row + d), col) for d in (1, 2, 3)]

    def copy(src, dst, send, recv, device):
        return pltpu.make_async_remote_copy(
            src_ref=src, dst_ref=dst, send_sem=send, recv_sem=recv, device_id=device, device_id_type=MESH
        )

    def push(ref, send, recv, device):
        copy(ref, ref, send, recv, device).start()

    def arrived(ref, recv):
        copy(ref, ref, sent1.at[0], recv, partner).wait_recv()

    def gone(ref, send):
        copy(ref, ref, send, core_sem.at[0, 0], partner).wait_send()

    def stripe(n, q, a_of, part=None):
        start, size = SPANS[q]
        if part is not None:
            size //= 2
            start += part * size
        return vbuf.at[n, core, b, a_of, :, pl.ds(start, size)]

    def line(n, q, b_of, part=None):
        start, size = SPANS[q]
        first, count = (0, SIDE) if part is None else (2 * part, 2)
        return vbuf.at[n, core, b_of, pl.ds(first, count), :, pl.ds(start, size)]

    def load(n):
        own = lambda start, size: vbuf.at[n, core, b, a, :, pl.ds(start, size)]
        return (
            pltpu.make_async_copy(v_in.at[PANELS - 1 - n], own(0, ROWS), load_sem.at[n, 0]),
            pltpu.make_async_copy(t_in.at[PANELS - 1 - n], own(ROWS, WIDTH), load_sem.at[n, 1]),
        )

    def wait_load(n):
        for one in load(n):
            one.wait()

    def first_send(n, q):
        push(stripe(n, q, a), sent1.at[n], near_sem.at[n, q, 0], up_a)
        push(stripe(n, q, a), sent1.at[n], near_sem.at[n, q, 1], down_a)

    def stage_a(n, q):
        arrived(stripe(n, q, a_prev), near_sem.at[n, q, 0])
        push(stripe(n, q, a_prev, 0), sent1.at[n], half_sem.at[n, q, 0], up_a)
        arrived(stripe(n, q, a_next), near_sem.at[n, q, 1])
        push(stripe(n, q, a_next, 1), sent1.at[n], half_sem.at[n, q, 1], down_a)

    def stage_b(n, q):
        arrived(stripe(n, q, a_far, 0), half_sem.at[n, q, 0])
        arrived(stripe(n, q, a_far, 1), half_sem.at[n, q, 1])
        push(line(n, q, b), sent2.at[n], row_sem.at[n, q, 0], up_b)
        push(line(n, q, b), sent2.at[n], row_sem.at[n, q, 1], down_b)
        push(line(n, q, b), sent3.at[n], core_sem.at[n, q], partner)

    def stage_c(n, q):
        arrived(line(n, q, b_prev), row_sem.at[n, q, 0])
        push(line(n, q, b_prev, 0), sent2.at[n], rowhalf_sem.at[n, q, 0], up_b)
        push(line(n, q, b_prev), sent3.at[n], core_sem.at[n, q], partner)
        arrived(line(n, q, b_next), row_sem.at[n, q, 1])
        push(line(n, q, b_next, 1), sent2.at[n], rowhalf_sem.at[n, q, 1], down_b)
        push(line(n, q, b_next), sent3.at[n], core_sem.at[n, q], partner)

    def stage_d(n, q):
        arrived(line(n, q, b_far, 0), rowhalf_sem.at[n, q, 0])
        arrived(line(n, q, b_far, 1), rowhalf_sem.at[n, q, 1])
        push(line(n, q, b_far), sent3.at[n], core_sem.at[n, q], partner)

    def stage_e(n, q):
        start, size = SPANS[q]
        arrived(vbuf.at[n, 1 - core, :, :, :, pl.ds(start, size)], core_sem.at[n, q])

    def pair(n, i, start, size):
        yy, xx = divmod(i, SIDE)
        lanes = pl.ds(start, size)
        return jnp.concatenate([vbuf[n, 0, yy, xx, :, lanes], vbuf[n, 1, xx, yy, :, lanes]], axis=0)

    def absorb(n, q):
        slot = lax.rem(n, 2)
        rows = pl.ds(CHUNK * q, CHUNK)
        for i in range(SIDE * SIDE):
            high, low = halves(pair(n, i, CHUNK * q, CHUNK))
            vh[pl.ds(2 * STRIPE * i, 2 * STRIPE), :] = high
            vl[pl.ds(2 * STRIPE * i, 2 * STRIPE), :] = low
        vnh[slot, rows, :] = vh[...].T
        vnl[slot, rows, :] = vl[...].T
        right = (
            jnp.concatenate([zh[rows, :], vnh[1 - slot, rows, :]], axis=1),
            jnp.concatenate([zl[rows, :], vnl[1 - slot, rows, :]], axis=1),
        )
        part = dot3((vh[...], vl[...]), right)
        both[...] = part if q == 0 else both[...] + part

    share = COLS // (2 * SIDE)

    def rows_of(wave, z_of):
        start = pl.multiple_of(wave * (COLS // 2) + share * z_of, share)
        return pl.ds(start, share)

    def take_s(n):
        for wave in (0, 1):
            for d in (1, 2, 3):
                arrived(sfull.at[n, rows_of(wave, wrap(row - d))], ag_sem.at[n, wave, d - 1])
        sh[...], sl[...] = halves(sfull[n].T)

    def finish(n):
        @pl.when(n == 0)
        def _():
            psend[n] = both[:, :COLS].T

        @pl.when(n > 0)
        def _():
            take_s(n - 1)
            psend[n] = (both[:, :COLS] - dot3(halves(both[:, COLS:]), (sh[...], sl[...]))).T

        for wave in (0, 1):
            for d in (2, 1, 3):
                src, dst = psend.at[n, rows_of(wave, wrap(row + d))], prec.at[n, wave, d - 1]
                copy(src, dst, rs_sent.at[n], rs_sem.at[n, wave, d - 1], lifts[d - 1]).start()

    def scale(n):
        factor = jnp.concatenate([pair(n, i, ROWS, WIDTH) for i in range(SIDE * SIDE)], axis=0)
        th[...], tl[...] = halves(factor)
        for wave in (0, 1):
            own = rows_of(wave, row)
            for d in (1, 3, 2):
                arrived(prec.at[n, wave, d - 1], rs_sem.at[n, wave, d - 1])
            total = psend[n, own, :] + prec[n, wave, 0] + prec[n, wave, 1] + prec[n, wave, 2]
            sfull[n, own, :] = dot3(halves(total), (th[...], tl[...]))
            for d in (2, 1, 3):
                push(sfull.at[n, own], ag_sent.at[n], ag_sem.at[n, wave, d - 1], lifts[d - 1])

    def update_rows(n, q):
        slot, rows = lax.rem(n, 2), pl.ds(CHUNK * q, CHUNK)
        new = z[rows, :] - dot3((vnh[slot, rows, :], vnl[slot, rows, :]), (sh[...], sl[...]))
        z[rows, :] = new
        zh[rows, :], zl[rows, :] = halves(new)

    def update(n, last=False):
        slot = lax.rem(n, 2)

        def body(i, carry):
            rows = pl.ds(pl.multiple_of(i * BLOCK, BLOCK), BLOCK)
            new = z[rows, :] - dot3((vnh[slot, rows, :], vnl[slot, rows, :]), (sh[...], sl[...]))
            z[rows, :] = new
            if not last:
                zh[rows, :], zl[rows, :] = halves(new)
            return carry

        lax.fori_loop(0, ROWS // BLOCK, body, 0)

    def near_chunk(m, q):
        @pl.when(m < PANELS)
        def _():
            if q == 0:
                wait_load(m)
            first_send(m, q)

    def near(p, q):
        at = lambda chunk: (chunk // QUARTERS, chunk % QUARTERS)
        if EARLY == 0:
            m, at_q = at(AHEAD + q)
            near_chunk(p + m, at_q)
            return

        @pl.when(p < EARLY)
        def _():
            for extra in (0, 1):
                m, at_q = at(AHEAD + 2 * q + extra)
                near_chunk(2 * p + m, at_q)

        @pl.when(p >= EARLY)
        def _():
            m, at_q = at(AHEAD + QUARTERS * EARLY + q)
            near_chunk(p + m, at_q)

    z_load = pltpu.make_async_copy(z_in, z, z_sem)

    def start_load(n, carry):
        for one in load(n):
            one.start()
        return carry

    lax.fori_loop(0, PANELS, start_load, 0)
    z_load.start()

    barrier = pltpu.get_barrier_semaphore()
    greeted = [up_a, down_a, up_b, down_b, partner] + lifts
    for device in greeted:
        pl.semaphore_signal(barrier, inc=1, device_id=device, device_id_type=MESH)
    pl.semaphore_wait(barrier, len(greeted))

    for chunk in range(AHEAD):
        near_chunk(jnp.int32(chunk // QUARTERS), chunk % QUARTERS)
    z_load.wait()

    def split_z(i, carry):
        rows = pl.ds(pl.multiple_of(i * BLOCK, BLOCK), BLOCK)
        zh[rows, :], zl[rows, :] = halves(z[rows, :])
        return carry

    lax.fori_loop(0, ROWS // BLOCK, split_z, 0)

    def panel(p, carry):
        def behind(q, lag):
            return p + (q - lag) // QUARTERS, (q - lag) % QUARTERS

        for q in range(QUARTERS):

            near(p, q)

            def run(stages):
                for lag, stage in stages:
                    m, at_q = behind(q, lag)
                    pl.when((m >= 0) & (m < PANELS))(lambda: stage(m, at_q))

            n, e_q = behind(q, LAGS[-1])
            live = (n >= 0) & (n < PANELS)

            def renew():
                pl.when(n > 1)(lambda: update_rows(n - 2, e_q))

            def work():
                stage_e(n, e_q)
                absorb(n, e_q)
                if e_q == 1:
                    pl.when(n > 0)(lambda: scale(n - 1))
                if e_q == QUARTERS - 1:
                    finish(n)

            A, B, C, D = zip(LAGS, (stage_a, stage_b, stage_c, stage_d))
            run((A, B))
            pl.when(live)(renew)
            run((C, D))
            pl.when(live)(work)

        return carry

    lax.fori_loop(0, PANELS + -(-LAGS[-1] // QUARTERS), panel, 0)

    update(PANELS - 2)
    scale(PANELS - 1)
    take_s(PANELS - 1)
    update(PANELS - 1, last=True)

    def close(n, carry):
        gone(vbuf.at[n, 0, 0, pl.ds(0, 3)], sent1.at[n])
        gone(vbuf.at[n, 0, pl.ds(0, 3)], sent2.at[n])
        gone(vbuf.at[n, 0], sent3.at[n])
        gone(prec.at[n], rs_sent.at[n])
        gone(prec.at[n], ag_sent.at[n])
        return carry

    lax.fori_loop(0, PANELS, close, 0)


def local(eigvecs, v_panels, t_panels):
    dma = pltpu.SemaphoreType.DMA
    anywhere = pl.BlockSpec(memory_space=pl.ANY)
    return pl.pallas_call(
        kernel,
        out_shape=pltpu.VMEM((ROWS, COLS), F32),
        in_specs=[anywhere] * 3,
        out_specs=pl.BlockSpec(memory_space=pltpu.VMEM),
        scratch_shapes=[
            pltpu.VMEM((PANELS, 2, SIDE, SIDE, STRIPE, LANES), F32),
            pltpu.VMEM((ROWS, COLS), BF16),
            pltpu.VMEM((ROWS, COLS), BF16),
            pltpu.VMEM((WIDTH, CHUNK), BF16),
            pltpu.VMEM((WIDTH, CHUNK), BF16),
            pltpu.VMEM((2, ROWS, WIDTH), BF16),
            pltpu.VMEM((2, ROWS, WIDTH), BF16),
            pltpu.VMEM((WIDTH, COLS + WIDTH), F32),
            pltpu.VMEM((PANELS, COLS, WIDTH), F32),
            pltpu.VMEM((PANELS, 2, 3, COLS // 8, WIDTH), F32),
            pltpu.VMEM((PANELS, COLS, WIDTH), F32),
            pltpu.VMEM((WIDTH, COLS), BF16),
            pltpu.VMEM((WIDTH, COLS), BF16),
            pltpu.VMEM((WIDTH, WIDTH), BF16),
            pltpu.VMEM((WIDTH, WIDTH), BF16),
            dma((PANELS, 2)),
            dma,
            dma((PANELS, QUARTERS, 2)),
            dma((PANELS, QUARTERS, 2)),
            dma((PANELS, QUARTERS, 2)),
            dma((PANELS, QUARTERS, 2)),
            dma((PANELS, QUARTERS)),
            dma((PANELS,)),
            dma((PANELS,)),
            dma((PANELS,)),
            dma((PANELS, 2, 3)),
            dma((PANELS,)),
            dma((PANELS, 2, 3)),
            dma((PANELS,)),
        ],
        compiler_params=pltpu.CompilerParams(
            collective_id=0, has_side_effects=True, vmem_limit_bytes=58 * 2**20
        ),
    )(eigvecs, jnp.swapaxes(v_panels, 1, 2), jnp.swapaxes(t_panels, 1, 2))


def solution(mesh):
    in_specs = (P("row", "col"), P(None, "row", "col"), P(None, None, "col"))
    out_specs = P("row", "col")
    return jax.shard_map(local, mesh=mesh, in_specs=in_specs, out_specs=out_specs, check_vma=False)
```

```python
import jax
import jax.numpy as jnp
from jax import lax
from jax.experimental import pallas as pl
from jax.experimental.pallas import tpu as pltpu
from jax.sharding import PartitionSpec as P

MESH = pl.DeviceIdType.MESH
F32, BF16 = jnp.float32, jnp.bfloat16
PANELS, WIDTH, ROWS, COLS = 8, 256, 4096, 256
SIDE, STRIPE = 4, 8
HALF = WIDTH // 2
CHUNK = 1024
SPANS = ((0, 1024), (1024, 1024), (2048, 1024), (3072, 1024))
QUARTERS = len(SPANS)
BLOCK = 1024
PIECES = 4
AHEAD = 3
EARLY = 1
LAGS = (0, 2, 4, 6, 7)


def halves(x):
    high = x.astype(BF16)
    return high, (x - high.astype(F32)).astype(BF16)


def dot3(left, right):
    (lh, ll), (rh, rl) = left, right
    dot = lambda u, v: jnp.dot(u, v, preferred_element_type=F32)
    return dot(lh, rh) + dot(lh, rl) + dot(ll, rh)


def kernel(
    z_in, v_in, t_in, z,
    vbuf, tbuf, tall, zh, zl, vh, vl, vnh, vnl, both, psend, prec, sfull, sh, sl, th, tl,
    load_sem, z_sem, tload_sem, t_sem, t_sent, lift_sem, liftpart_sem, swap_sem, lift_sent, swap_sent,
    near_sem, half_sem, row_sem, rowhalf_sem, core_sem, sent1, sent2, sent3,
    rs_sem, rs_sent, ag_sem, ag_sent,
):
    row, col = lax.axis_index("row"), lax.axis_index("col")
    core, x, y = lax.rem(col, 2), lax.rem(col // 2, SIDE), col // (2 * SIDE)
    a, b = x + core * (y - x), y + core * (x - y)
    step_a, step_b = 1 + 3 * core, 4 - 3 * core
    wrap = lambda i: lax.rem(i + SIDE, SIDE)

    def at(a_to, b_to):
        return (row, 2 * (a_to * step_a + b_to * step_b) + core)

    a_next, a_prev, b_next, b_prev = wrap(a + 1), wrap(a - 1), wrap(b + 1), wrap(b - 1)
    a_far, b_far = wrap(a + 2), wrap(b + 2)
    up_a, down_a, up_b, down_b = at(a_next, b), at(a_prev, b), at(a, b_next), at(a, b_prev)
    partner = (row, col + 1 - 2 * core)
    lifts = [(wrap(row + d), col) for d in (1, 2, 3)]

    def copy(src, dst, send, recv, device):
        return pltpu.make_async_remote_copy(
            src_ref=src, dst_ref=dst, send_sem=send, recv_sem=recv, device_id=device, device_id_type=MESH
        )

    def push(ref, send, recv, device):
        copy(ref, ref, send, recv, device).start()

    def arrived(ref, recv):
        copy(ref, ref, sent1.at[0], recv, partner).wait_recv()

    def gone(ref, send):
        copy(ref, ref, send, core_sem.at[0, 0], partner).wait_send()

    class Vectors:
        def __init__(self, n, q):
            self.n, self.span = n, SPANS[q]
            self.near = [near_sem.at[n, q, i] for i in (0, 1)]
            self.half = [half_sem.at[n, q, i] for i in (0, 1)]
            self.row = [row_sem.at[n, q, i] for i in (0, 1)]
            self.rowhalf = [rowhalf_sem.at[n, q, i] for i in (0, 1)]
            self.core, self.sent = core_sem.at[n, q], (sent1.at[n], sent2.at[n], sent3.at[n])

        def stripe(self, a_of, part=None):
            start, size = self.span
            if part is not None:
                size //= 2
                start += part * size
            return vbuf.at[self.n, core, b, a_of, :, pl.ds(start, size)]

        def line(self, b_of, part=None):
            first, count = (0, SIDE) if part is None else (2 * part, 2)
            return vbuf.at[self.n, core, b_of, pl.ds(first, count), :, pl.ds(*self.span)]

        def theirs(self):
            return vbuf.at[self.n, 1 - core, :, :, :, pl.ds(*self.span)]

    class Factors:
        near, half, row, rowhalf = [[t_sem.at[2 * j + i] for i in (0, 1)] for j in range(4)]
        core, sent = t_sem.at[8], (t_sent.at[0], t_sent.at[1], t_sent.at[2])

        def stripe(self, a_of, part=None):
            return tbuf.at[core, b, a_of, pl.ds(0, 2) if part is None else pl.ds(part, 1)]

        def line(self, b_of, part=None):
            first, count = (0, SIDE) if part is None else (2 * part, 2)
            return tbuf.at[core, b_of, pl.ds(first, count)]

        def theirs(self):
            return tbuf.at[1 - core]

    factors = Factors()

    def load(n):
        return (pltpu.make_async_copy(v_in.at[PANELS - 1 - n], vbuf.at[n, core, b, a], load_sem.at[n]),)

    def load_t(g):
        return pltpu.make_async_copy(t_in.at[PANELS - 1 - SIDE * g - row], tbuf.at[core, b, a, g], tload_sem.at[g])

    def wait_load(n):
        for one in load(n):
            one.wait()

    def first_send(s):
        push(s.stripe(a), s.sent[0], s.near[0], up_a)
        push(s.stripe(a), s.sent[0], s.near[1], down_a)

    def stage_a(s):
        arrived(s.stripe(a_prev), s.near[0])
        push(s.stripe(a_prev, 0), s.sent[0], s.half[0], up_a)
        arrived(s.stripe(a_next), s.near[1])
        push(s.stripe(a_next, 1), s.sent[0], s.half[1], down_a)

    def stage_b(s):
        arrived(s.stripe(a_far, 0), s.half[0])
        arrived(s.stripe(a_far, 1), s.half[1])
        push(s.line(b), s.sent[1], s.row[0], up_b)
        push(s.line(b), s.sent[1], s.row[1], down_b)
        push(s.line(b), s.sent[2], s.core, partner)

    def stage_c(s):
        arrived(s.line(b_prev), s.row[0])
        push(s.line(b_prev, 0), s.sent[1], s.rowhalf[0], up_b)
        push(s.line(b_prev), s.sent[2], s.core, partner)
        arrived(s.line(b_next), s.row[1])
        push(s.line(b_next, 1), s.sent[1], s.rowhalf[1], down_b)
        push(s.line(b_next), s.sent[2], s.core, partner)

    def stage_d(s):
        arrived(s.line(b_far, 0), s.rowhalf[0])
        arrived(s.line(b_far, 1), s.rowhalf[1])
        push(s.line(b_far), s.sent[2], s.core, partner)

    def stage_e(s):
        arrived(s.theirs(), s.core)

    def mine(g, z_of, of_core, piece=None):
        rows = HALF if piece is None else HALF // PIECES
        start = of_core * HALF + (0 if piece is None else piece * rows)
        return tall.at[SIDE * g + z_of, pl.ds(pl.multiple_of(start, rows), rows)]

    def lift_early():
        stage_e(factors)
        for g in (0, 1):
            for i in range(SIDE * SIDE):
                yy, xx = divmod(i, SIDE)
                both_cores = jnp.concatenate([tbuf[0, yy, xx, g], tbuf[1, xx, yy, g]], axis=0)
                tall[SIDE * g + row, pl.ds(2 * STRIPE * i, 2 * STRIPE), :] = both_cores
        for d in (2, 1, 3):
            push(mine(0, row, core), lift_sent.at[0], lift_sem.at[d - 1], lifts[d - 1])

    def lift_late(piece):
        for d in (2, 1, 3):
            push(mine(1, row, core, piece), lift_sent.at[1], liftpart_sem.at[piece, d - 1], lifts[d - 1])

    def swap(g):
        for d in (1, 2, 3):
            z_of = wrap(row - d)
            if g == 0:
                arrived(mine(0, z_of, core), lift_sem.at[d - 1])
            else:
                for piece in range(PIECES):
                    arrived(mine(1, z_of, core, piece), liftpart_sem.at[piece, d - 1])
            push(mine(g, z_of, core), swap_sent.at[g], swap_sem.at[g, d - 1], partner)

    def swapped(g):
        for d in (1, 2, 3):
            arrived(mine(g, wrap(row - d), 1 - core), swap_sem.at[g, d - 1])

    def pair(n, i, start, size):
        yy, xx = divmod(i, SIDE)
        lanes = pl.ds(start, size)
        return jnp.concatenate([vbuf[n, 0, yy, xx, :, lanes], vbuf[n, 1, xx, yy, :, lanes]], axis=0)

    def absorb(n, q):
        slot = lax.rem(n, 2)
        rows = pl.ds(CHUNK * q, CHUNK)
        for i in range(SIDE * SIDE):
            high, low = halves(pair(n, i, CHUNK * q, CHUNK))
            vh[pl.ds(2 * STRIPE * i, 2 * STRIPE), :] = high
            vl[pl.ds(2 * STRIPE * i, 2 * STRIPE), :] = low
        vnh[slot, rows, :] = vh[...].T
        vnl[slot, rows, :] = vl[...].T
        right = (
            jnp.concatenate([zh[rows, :], vnh[1 - slot, rows, :]], axis=1),
            jnp.concatenate([zl[rows, :], vnl[1 - slot, rows, :]], axis=1),
        )
        part = dot3((vh[...], vl[...]), right)
        both[...] = part if q == 0 else both[...] + part

    share = COLS // (2 * SIDE)

    def rows_of(wave, z_of):
        start = pl.multiple_of(wave * (COLS // 2) + share * z_of, share)
        return pl.ds(start, share)

    def take_s(n):
        for wave in (0, 1):
            for d in (1, 2, 3):
                arrived(sfull.at[n, rows_of(wave, wrap(row - d))], ag_sem.at[n, wave, d - 1])
        sh[...], sl[...] = halves(sfull[n].T)

    def finish(n):
        @pl.when(n == 0)
        def _():
            psend[n] = both[:, :COLS].T

        @pl.when(n > 0)
        def _():
            take_s(n - 1)
            psend[n] = (both[:, :COLS] - dot3(halves(both[:, COLS:]), (sh[...], sl[...]))).T

        for wave in (0, 1):
            for d in (2, 1, 3):
                src, dst = psend.at[n, rows_of(wave, wrap(row + d))], prec.at[n, wave, d - 1]
                copy(src, dst, rs_sent.at[n], rs_sem.at[n, wave, d - 1], lifts[d - 1]).start()

    def scale(n):
        pl.when(n == 0)(lambda: swapped(0))
        pl.when(n == SIDE)(lambda: swapped(1))
        th[...], tl[...] = halves(tall[n])
        for wave in (0, 1):
            own = rows_of(wave, row)
            for d in (1, 3, 2):
                arrived(prec.at[n, wave, d - 1], rs_sem.at[n, wave, d - 1])
            total = psend[n, own, :] + prec[n, wave, 0] + prec[n, wave, 1] + prec[n, wave, 2]
            sfull[n, own, :] = dot3(halves(total), (th[...], tl[...]))
            for d in (2, 1, 3):
                push(sfull.at[n, own], ag_sent.at[n], ag_sem.at[n, wave, d - 1], lifts[d - 1])

    def update_rows(n, q):
        slot, rows = lax.rem(n, 2), pl.ds(CHUNK * q, CHUNK)
        new = z[rows, :] - dot3((vnh[slot, rows, :], vnl[slot, rows, :]), (sh[...], sl[...]))
        z[rows, :] = new
        zh[rows, :], zl[rows, :] = halves(new)

    def update(n, last=False):
        slot = lax.rem(n, 2)

        def body(i, carry):
            rows = pl.ds(pl.multiple_of(i * BLOCK, BLOCK), BLOCK)
            new = z[rows, :] - dot3((vnh[slot, rows, :], vnl[slot, rows, :]), (sh[...], sl[...]))
            z[rows, :] = new
            if not last:
                zh[rows, :], zl[rows, :] = halves(new)
            return carry

        lax.fori_loop(0, ROWS // BLOCK, body, 0)

    def near_chunk(m, q):
        @pl.when(m < PANELS)
        def _():
            if q == 0:
                wait_load(m)
            first_send(Vectors(m, q))

    def near(p, q):
        at = lambda chunk: (chunk // QUARTERS, chunk % QUARTERS)
        if EARLY == 0:
            m, at_q = at(AHEAD + q)
            near_chunk(p + m, at_q)
            return

        @pl.when(p < EARLY)
        def _():
            for extra in (0, 1):
                m, at_q = at(AHEAD + 2 * q + extra)
                near_chunk(2 * p + m, at_q)

        @pl.when(p >= EARLY)
        def _():
            m, at_q = at(AHEAD + QUARTERS * EARLY + q)
            near_chunk(p + m, at_q)

    z_load = pltpu.make_async_copy(z_in, z, z_sem)

    def start_load(n, carry):
        for one in load(n):
            one.start()
        return carry

    for g in (0, 1):
        load_t(g).start()
    lax.fori_loop(0, PANELS, start_load, 0)
    z_load.start()

    barrier = pltpu.get_barrier_semaphore()
    greeted = [up_a, down_a, up_b, down_b, partner] + lifts
    for device in greeted:
        pl.semaphore_signal(barrier, inc=1, device_id=device, device_id_type=MESH)
    pl.semaphore_wait(barrier, len(greeted))

    for g in (0, 1):
        load_t(g).wait()
    first_send(factors)
    for chunk in range(AHEAD):
        near_chunk(jnp.int32(chunk // QUARTERS), chunk % QUARTERS)
    z_load.wait()

    def split_z(i, carry):
        rows = pl.ds(pl.multiple_of(i * BLOCK, BLOCK), BLOCK)
        zh[rows, :], zl[rows, :] = halves(z[rows, :])
        return carry

    lax.fori_loop(0, ROWS // BLOCK, split_z, 0)

    def panel(p, carry):
        def behind(q, lag):
            return p + (q - lag) // QUARTERS, (q - lag) % QUARTERS

        for q in range(QUARTERS):

            near(p, q)

            def run(stages):
                for lag, stage in stages:
                    if lag % QUARTERS == q:
                        pl.when(p == lag // QUARTERS)(lambda: stage(factors))
                    m, at_q = behind(q, lag)
                    pl.when((m >= 0) & (m < PANELS))(lambda: stage(Vectors(m, at_q)))

            n, e_q = behind(q, LAGS[-1])
            live = (n >= 0) & (n < PANELS)

            def renew():
                pl.when(n > 1)(lambda: update_rows(n - 2, e_q))

            def work():
                stage_e(Vectors(n, e_q))
                absorb(n, e_q)
                if e_q == 1:
                    pl.when(n > 0)(lambda: scale(n - 1))
                if e_q == QUARTERS - 1:
                    finish(n)

            A, B, C, D = zip(LAGS, (stage_a, stage_b, stage_c, stage_d))
            run((B, A))
            pl.when(live)(renew)
            run((D, C))
            if q == LAGS[-1] % QUARTERS:
                pl.when(p == LAGS[-1] // QUARTERS)(lift_early)
            pl.when(live)(work)
            if q == 1:
                for piece in range(PIECES):
                    pl.when(p == 2 + piece)(lambda: lift_late(piece))
            if q == QUARTERS - 1:
                pl.when(p == 2)(lambda: swap(0))
                pl.when(p == 6)(lambda: swap(1))

        return carry

    lax.fori_loop(0, PANELS + -(-LAGS[-1] // QUARTERS), panel, 0)

    update(PANELS - 2)
    scale(PANELS - 1)
    take_s(PANELS - 1)
    update(PANELS - 1, last=True)

    def close(n, carry):
        gone(vbuf.at[n, 0, 0, pl.ds(0, 3)], sent1.at[n])
        gone(vbuf.at[n, 0, pl.ds(0, 3)], sent2.at[n])
        gone(vbuf.at[n, 0], sent3.at[n])
        gone(prec.at[n], rs_sent.at[n])
        gone(prec.at[n], ag_sent.at[n])
        return carry

    lax.fori_loop(0, PANELS, close, 0)
    gone(tbuf.at[0, 0, pl.ds(0, 3)], t_sent.at[0])
    gone(tbuf.at[0, pl.ds(0, 3)], t_sent.at[1])
    gone(tbuf.at[0], t_sent.at[2])
    for g in (0, 1):
        gone(tall.at[pl.ds(0, 3), pl.ds(0, HALF)], lift_sent.at[g])
        gone(tall.at[pl.ds(0, 3), pl.ds(0, HALF)], swap_sent.at[g])


def local(eigvecs, v_panels, t_panels):
    dma = pltpu.SemaphoreType.DMA
    anywhere = pl.BlockSpec(memory_space=pl.ANY)
    return pl.pallas_call(
        kernel,
        out_shape=pltpu.VMEM((ROWS, COLS), F32),
        in_specs=[anywhere] * 3,
        out_specs=pl.BlockSpec(memory_space=pltpu.VMEM),
        scratch_shapes=[
            pltpu.VMEM((PANELS, 2, SIDE, SIDE, STRIPE, ROWS), F32),
            pltpu.VMEM((2, SIDE, SIDE, 2, STRIPE, WIDTH), F32),
            pltpu.VMEM((PANELS, WIDTH, WIDTH), F32),
            pltpu.VMEM((ROWS, COLS), BF16),
            pltpu.VMEM((ROWS, COLS), BF16),
            pltpu.VMEM((WIDTH, CHUNK), BF16),
            pltpu.VMEM((WIDTH, CHUNK), BF16),
            pltpu.VMEM((2, ROWS, WIDTH), BF16),
            pltpu.VMEM((2, ROWS, WIDTH), BF16),
            pltpu.VMEM((WIDTH, COLS + WIDTH), F32),
            pltpu.VMEM((PANELS, COLS, WIDTH), F32),
            pltpu.VMEM((PANELS, 2, 3, COLS // 8, WIDTH), F32),
            pltpu.VMEM((PANELS, COLS, WIDTH), F32),
            pltpu.VMEM((WIDTH, COLS), BF16),
            pltpu.VMEM((WIDTH, COLS), BF16),
            pltpu.VMEM((WIDTH, WIDTH), BF16),
            pltpu.VMEM((WIDTH, WIDTH), BF16),
            dma((PANELS,)),
            dma,
            dma((2,)),
            dma((9,)),
            dma((3,)),
            dma((3,)),
            dma((PIECES, 3)),
            dma((2, 3)),
            dma((2,)),
            dma((2,)),
            dma((PANELS, QUARTERS, 2)),
            dma((PANELS, QUARTERS, 2)),
            dma((PANELS, QUARTERS, 2)),
            dma((PANELS, QUARTERS, 2)),
            dma((PANELS, QUARTERS)),
            dma((PANELS,)),
            dma((PANELS,)),
            dma((PANELS,)),
            dma((PANELS, 2, 3)),
            dma((PANELS,)),
            dma((PANELS, 2, 3)),
            dma((PANELS,)),
        ],
        compiler_params=pltpu.CompilerParams(
            collective_id=0, has_side_effects=True, vmem_limit_bytes=58 * 2**20
        ),
    )(eigvecs, jnp.swapaxes(v_panels, 1, 2), jnp.swapaxes(t_panels, 1, 2))


def solution(mesh):
    in_specs = (P("row", "col"), P(None, "row", "col"), P(None, None, "col"))
    out_specs = P("row", "col")
    return jax.shard_map(local, mesh=mesh, in_specs=in_specs, out_specs=out_specs, check_vma=False)
```

```python
import jax
import jax.numpy as jnp
from jax import lax
from jax.experimental import pallas as pl
from jax.experimental.pallas import tpu as pltpu
from jax.sharding import PartitionSpec as P

MESH = pl.DeviceIdType.MESH
F32, BF16 = jnp.float32, jnp.bfloat16
PANELS, WIDTH, ROWS, COLS = 8, 256, 4096, 256
SIDE, STRIPE = 4, 8
HALF = WIDTH // 2
CHUNK = 1024
SPANS = ((0, 1024), (1024, 1024), (2048, 1024), (3072, 1024))
QUARTERS = len(SPANS)
BLOCK = 1024
PIECES = 4
BAND = 1024
AHEAD = 3
EARLY = 1
LAGS = (0, 2, 4, 6, 7)


def halves(x):
    high = x.astype(BF16)
    return high, (x - high.astype(F32)).astype(BF16)


def dot3(left, right):
    (lh, ll), (rh, rl) = left, right
    dot = lambda u, v: jnp.dot(u, v, preferred_element_type=F32)
    return dot(lh, rh) + dot(lh, rl) + dot(ll, rh)


def kernel(
    z_in, v_in, t_in, z, vnh, vnl, sh, sl,
    vbuf, tbuf, tall, zh, zl, vh, vl, both, psend, prec, sfull, th, tl,
    load_sem, z_sem, tload_sem, t_sem, t_sent, lift_sem, liftpart_sem, swap_sem, lift_sent, swap_sent,
    near_sem, half_sem, row_sem, rowhalf_sem, core_sem, sent1, sent2, sent3,
    rs_sem, rs_sent, ag_sem, ag_sent,
):
    row, col = lax.axis_index("row"), lax.axis_index("col")
    core, x, y = lax.rem(col, 2), lax.rem(col // 2, SIDE), col // (2 * SIDE)
    a, b = x + core * (y - x), y + core * (x - y)
    step_a, step_b = 1 + 3 * core, 4 - 3 * core
    wrap = lambda i: lax.rem(i + SIDE, SIDE)

    def at(a_to, b_to):
        return (row, 2 * (a_to * step_a + b_to * step_b) + core)

    a_next, a_prev, b_next, b_prev = wrap(a + 1), wrap(a - 1), wrap(b + 1), wrap(b - 1)
    a_far, b_far = wrap(a + 2), wrap(b + 2)
    up_a, down_a, up_b, down_b = at(a_next, b), at(a_prev, b), at(a, b_next), at(a, b_prev)
    partner = (row, col + 1 - 2 * core)
    lifts = [(wrap(row + d), col) for d in (1, 2, 3)]

    def copy(src, dst, send, recv, device):
        return pltpu.make_async_remote_copy(
            src_ref=src, dst_ref=dst, send_sem=send, recv_sem=recv, device_id=device, device_id_type=MESH
        )

    def push(ref, send, recv, device):
        copy(ref, ref, send, recv, device).start()

    def arrived(ref, recv):
        copy(ref, ref, sent1.at[0], recv, partner).wait_recv()

    def gone(ref, send):
        copy(ref, ref, send, core_sem.at[0, 0], partner).wait_send()

    class Vectors:
        def __init__(self, n, q):
            self.n, self.span = n, SPANS[q]
            self.near = [near_sem.at[n, q, i] for i in (0, 1)]
            self.half = [half_sem.at[n, q, i] for i in (0, 1)]
            self.row = [row_sem.at[n, q, i] for i in (0, 1)]
            self.rowhalf = [rowhalf_sem.at[n, q, i] for i in (0, 1)]
            self.core, self.sent = core_sem.at[n, q], (sent1.at[n], sent2.at[n], sent3.at[n])

        def stripe(self, a_of, part=None):
            start, size = self.span
            if part is not None:
                size //= 2
                start += part * size
            return vbuf.at[self.n, core, b, a_of, :, pl.ds(start, size)]

        def line(self, b_of, part=None):
            first, count = (0, SIDE) if part is None else (2 * part, 2)
            return vbuf.at[self.n, core, b_of, pl.ds(first, count), :, pl.ds(*self.span)]

        def theirs(self):
            return vbuf.at[self.n, 1 - core, :, :, :, pl.ds(*self.span)]

    class Factors:
        near, half, row, rowhalf = [[t_sem.at[2 * j + i] for i in (0, 1)] for j in range(4)]
        core, sent = t_sem.at[8], (t_sent.at[0], t_sent.at[1], t_sent.at[2])

        def stripe(self, a_of, part=None):
            return tbuf.at[core, b, a_of, pl.ds(0, 2) if part is None else pl.ds(part, 1)]

        def line(self, b_of, part=None):
            first, count = (0, SIDE) if part is None else (2 * part, 2)
            return tbuf.at[core, b_of, pl.ds(first, count)]

        def theirs(self):
            return tbuf.at[1 - core]

    factors = Factors()

    def load(n):
        return (pltpu.make_async_copy(v_in.at[PANELS - 1 - n], vbuf.at[n, core, b, a], load_sem.at[n]),)

    def load_t(g):
        return pltpu.make_async_copy(t_in.at[PANELS - 1 - SIDE * g - row], tbuf.at[core, b, a, g], tload_sem.at[g])

    def wait_load(n):
        for one in load(n):
            one.wait()

    def first_send(s):
        push(s.stripe(a), s.sent[0], s.near[0], up_a)
        push(s.stripe(a), s.sent[0], s.near[1], down_a)

    def stage_a(s):
        arrived(s.stripe(a_prev), s.near[0])
        push(s.stripe(a_prev, 0), s.sent[0], s.half[0], up_a)
        arrived(s.stripe(a_next), s.near[1])
        push(s.stripe(a_next, 1), s.sent[0], s.half[1], down_a)

    def stage_b(s):
        arrived(s.stripe(a_far, 0), s.half[0])
        arrived(s.stripe(a_far, 1), s.half[1])
        push(s.line(b), s.sent[1], s.row[0], up_b)
        push(s.line(b), s.sent[1], s.row[1], down_b)
        push(s.line(b), s.sent[2], s.core, partner)

    def stage_c(s):
        arrived(s.line(b_prev), s.row[0])
        push(s.line(b_prev, 0), s.sent[1], s.rowhalf[0], up_b)
        push(s.line(b_prev), s.sent[2], s.core, partner)
        arrived(s.line(b_next), s.row[1])
        push(s.line(b_next, 1), s.sent[1], s.rowhalf[1], down_b)
        push(s.line(b_next), s.sent[2], s.core, partner)

    def stage_d(s):
        arrived(s.line(b_far, 0), s.rowhalf[0])
        arrived(s.line(b_far, 1), s.rowhalf[1])
        push(s.line(b_far), s.sent[2], s.core, partner)

    def stage_e(s):
        arrived(s.theirs(), s.core)

    def mine(g, z_of, of_core, piece=None):
        rows = HALF if piece is None else HALF // PIECES
        start = of_core * HALF + (0 if piece is None else piece * rows)
        return tall.at[SIDE * g + z_of, pl.ds(pl.multiple_of(start, rows), rows)]

    def lift_early():
        stage_e(factors)
        for g in (0, 1):
            for i in range(SIDE * SIDE):
                yy, xx = divmod(i, SIDE)
                both_cores = jnp.concatenate([tbuf[0, yy, xx, g], tbuf[1, xx, yy, g]], axis=0)
                tall[SIDE * g + row, pl.ds(2 * STRIPE * i, 2 * STRIPE), :] = both_cores
        for d in (2, 1, 3):
            push(mine(0, row, core), lift_sent.at[0], lift_sem.at[d - 1], lifts[d - 1])

    def lift_late(piece):
        for d in (2, 1, 3):
            push(mine(1, row, core, piece), lift_sent.at[1], liftpart_sem.at[piece, d - 1], lifts[d - 1])

    def swap(g):
        for d in (1, 2, 3):
            z_of = wrap(row - d)
            if g == 0:
                arrived(mine(0, z_of, core), lift_sem.at[d - 1])
            else:
                for piece in range(PIECES):
                    arrived(mine(1, z_of, core, piece), liftpart_sem.at[piece, d - 1])
            push(mine(g, z_of, core), swap_sent.at[g], swap_sem.at[g, d - 1], partner)

    def swapped(g):
        for d in (1, 2, 3):
            arrived(mine(g, wrap(row - d), 1 - core), swap_sem.at[g, d - 1])

    def pair(n, i, start, size):
        yy, xx = divmod(i, SIDE)
        lanes = pl.ds(start, size)
        return jnp.concatenate([vbuf[n, 0, yy, xx, :, lanes], vbuf[n, 1, xx, yy, :, lanes]], axis=0)

    def absorb(n, q):
        slot = lax.rem(n, 2)
        rows = pl.ds(CHUNK * q, CHUNK)
        for i in range(SIDE * SIDE):
            high, low = halves(pair(n, i, CHUNK * q, CHUNK))
            vh[pl.ds(2 * STRIPE * i, 2 * STRIPE), :] = high
            vl[pl.ds(2 * STRIPE * i, 2 * STRIPE), :] = low
        vnh[slot, rows, :] = vh[...].T
        vnl[slot, rows, :] = vl[...].T
        right = (
            jnp.concatenate([zh[rows, :], vnh[1 - slot, rows, :]], axis=1),
            jnp.concatenate([zl[rows, :], vnl[1 - slot, rows, :]], axis=1),
        )
        part = dot3((vh[...], vl[...]), right)
        both[...] = part if q == 0 else both[...] + part

    share = COLS // (2 * SIDE)

    def rows_of(wave, z_of):
        start = pl.multiple_of(wave * (COLS // 2) + share * z_of, share)
        return pl.ds(start, share)

    def take_s(n):
        for wave in (0, 1):
            for d in (1, 2, 3):
                arrived(sfull.at[n, rows_of(wave, wrap(row - d))], ag_sem.at[n, wave, d - 1])
        sh[...], sl[...] = halves(sfull[n].T)

    def finish(n):
        @pl.when(n == 0)
        def _():
            psend[n] = both[:, :COLS].T

        @pl.when(n > 0)
        def _():
            take_s(n - 1)
            psend[n] = (both[:, :COLS] - dot3(halves(both[:, COLS:]), (sh[...], sl[...]))).T

        for wave in (0, 1):
            for d in (2, 1, 3):
                src, dst = psend.at[n, rows_of(wave, wrap(row + d))], prec.at[n, wave, d - 1]
                copy(src, dst, rs_sent.at[n], rs_sem.at[n, wave, d - 1], lifts[d - 1]).start()

    def scale(n):
        pl.when(n == 0)(lambda: swapped(0))
        pl.when(n == SIDE)(lambda: swapped(1))
        th[...], tl[...] = halves(tall[n])
        for wave in (0, 1):
            own = rows_of(wave, row)
            for d in (1, 3, 2):
                arrived(prec.at[n, wave, d - 1], rs_sem.at[n, wave, d - 1])
            total = psend[n, own, :] + prec[n, wave, 0] + prec[n, wave, 1] + prec[n, wave, 2]
            sfull[n, own, :] = dot3(halves(total), (th[...], tl[...]))
            for d in (2, 1, 3):
                push(sfull.at[n, own], ag_sent.at[n], ag_sem.at[n, wave, d - 1], lifts[d - 1])

    def update_rows(n, q):
        slot, rows = lax.rem(n, 2), pl.ds(CHUNK * q, CHUNK)
        new = z[rows, :] - dot3((vnh[slot, rows, :], vnl[slot, rows, :]), (sh[...], sl[...]))
        z[rows, :] = new
        zh[rows, :], zl[rows, :] = halves(new)

    def update(n, last=False):
        slot = lax.rem(n, 2)

        def body(i, carry):
            rows = pl.ds(pl.multiple_of(i * BLOCK, BLOCK), BLOCK)
            new = z[rows, :] - dot3((vnh[slot, rows, :], vnl[slot, rows, :]), (sh[...], sl[...]))
            z[rows, :] = new
            if not last:
                zh[rows, :], zl[rows, :] = halves(new)
            return carry

        lax.fori_loop(0, ROWS // BLOCK, body, 0)

    def near_chunk(m, q):
        @pl.when(m < PANELS)
        def _():
            if q == 0:
                wait_load(m)
            first_send(Vectors(m, q))

    def near(p, q):
        at = lambda chunk: (chunk // QUARTERS, chunk % QUARTERS)
        if EARLY == 0:
            m, at_q = at(AHEAD + q)
            near_chunk(p + m, at_q)
            return

        @pl.when(p < EARLY)
        def _():
            for extra in (0, 1):
                m, at_q = at(AHEAD + 2 * q + extra)
                near_chunk(2 * p + m, at_q)

        @pl.when(p >= EARLY)
        def _():
            m, at_q = at(AHEAD + QUARTERS * EARLY + q)
            near_chunk(p + m, at_q)

    z_load = pltpu.make_async_copy(z_in, z, z_sem)

    def start_load(n, carry):
        for one in load(n):
            one.start()
        return carry

    for g in (0, 1):
        load_t(g).start()
    lax.fori_loop(0, PANELS, start_load, 0)
    z_load.start()

    barrier = pltpu.get_barrier_semaphore()
    greeted = [up_a, down_a, up_b, down_b, partner] + lifts
    for device in greeted:
        pl.semaphore_signal(barrier, inc=1, device_id=device, device_id_type=MESH)
    pl.semaphore_wait(barrier, len(greeted))

    for g in (0, 1):
        load_t(g).wait()
    first_send(factors)
    for chunk in range(AHEAD):
        near_chunk(jnp.int32(chunk // QUARTERS), chunk % QUARTERS)
    z_load.wait()

    def split_z(i, carry):
        rows = pl.ds(pl.multiple_of(i * BLOCK, BLOCK), BLOCK)
        zh[rows, :], zl[rows, :] = halves(z[rows, :])
        return carry

    lax.fori_loop(0, ROWS // BLOCK, split_z, 0)

    def panel(p, carry):
        def behind(q, lag):
            return p + (q - lag) // QUARTERS, (q - lag) % QUARTERS

        for q in range(QUARTERS):

            near(p, q)

            def run(stages):
                for lag, stage in stages:
                    if lag % QUARTERS == q:
                        pl.when(p == lag // QUARTERS)(lambda: stage(factors))
                    m, at_q = behind(q, lag)
                    pl.when((m >= 0) & (m < PANELS))(lambda: stage(Vectors(m, at_q)))

            n, e_q = behind(q, LAGS[-1])
            live = (n >= 0) & (n < PANELS)

            def renew():
                pl.when(n > 1)(lambda: update_rows(n - 2, e_q))

            def work():
                stage_e(Vectors(n, e_q))
                absorb(n, e_q)
                if e_q == 1:
                    pl.when(n > 0)(lambda: scale(n - 1))
                if e_q == QUARTERS - 1:
                    finish(n)

            A, B, C, D = zip(LAGS, (stage_a, stage_b, stage_c, stage_d))
            run((B, A))
            pl.when(live)(renew)
            run((D, C))
            if q == LAGS[-1] % QUARTERS:
                pl.when(p == LAGS[-1] // QUARTERS)(lift_early)
            pl.when(live)(work)
            if q == 1:
                for piece in range(PIECES):
                    pl.when(p == 2 + piece)(lambda: lift_late(piece))
            if q == QUARTERS - 1:
                pl.when(p == 2)(lambda: swap(0))
                pl.when(p == 6)(lambda: swap(1))

        return carry

    lax.fori_loop(0, PANELS + -(-LAGS[-1] // QUARTERS), panel, 0)

    update(PANELS - 2)
    scale(PANELS - 1)
    take_s(PANELS - 1)

    def close(n, carry):
        gone(vbuf.at[n, 0, 0, pl.ds(0, 3)], sent1.at[n])
        gone(vbuf.at[n, 0, pl.ds(0, 3)], sent2.at[n])
        gone(vbuf.at[n, 0], sent3.at[n])
        gone(prec.at[n], rs_sent.at[n])
        gone(prec.at[n], ag_sent.at[n])
        return carry

    lax.fori_loop(0, PANELS, close, 0)
    gone(tbuf.at[0, 0, pl.ds(0, 3)], t_sent.at[0])
    gone(tbuf.at[0, pl.ds(0, 3)], t_sent.at[1])
    gone(tbuf.at[0], t_sent.at[2])
    for g in (0, 1):
        gone(tall.at[pl.ds(0, 3), pl.ds(0, HALF)], lift_sent.at[g])
        gone(tall.at[pl.ds(0, 3), pl.ds(0, HALF)], swap_sent.at[g])


def last_update(z, vnh, vnl, sh, sl, out):
    rows = pl.ds(pl.multiple_of(pl.program_id(0) * BAND, BAND), BAND)
    slot = (PANELS - 1) % 2
    out[...] = z[rows, :] - dot3((vnh[slot, rows, :], vnl[slot, rows, :]), (sh[...], sl[...]))


def local(eigvecs, v_panels, t_panels):
    dma = pltpu.SemaphoreType.DMA
    anywhere = pl.BlockSpec(memory_space=pl.ANY)
    state = pl.pallas_call(
        kernel,
        out_shape=(
            pltpu.VMEM((ROWS, COLS), F32),
            pltpu.VMEM((2, ROWS, WIDTH), BF16),
            pltpu.VMEM((2, ROWS, WIDTH), BF16),
            pltpu.VMEM((WIDTH, COLS), BF16),
            pltpu.VMEM((WIDTH, COLS), BF16),
        ),
        in_specs=[anywhere] * 3,
        out_specs=(pl.BlockSpec(memory_space=pltpu.VMEM),) * 5,
        scratch_shapes=[
            pltpu.VMEM((PANELS, 2, SIDE, SIDE, STRIPE, ROWS), F32),
            pltpu.VMEM((2, SIDE, SIDE, 2, STRIPE, WIDTH), F32),
            pltpu.VMEM((PANELS, WIDTH, WIDTH), F32),
            pltpu.VMEM((ROWS, COLS), BF16),
            pltpu.VMEM((ROWS, COLS), BF16),
            pltpu.VMEM((WIDTH, CHUNK), BF16),
            pltpu.VMEM((WIDTH, CHUNK), BF16),
            pltpu.VMEM((WIDTH, COLS + WIDTH), F32),
            pltpu.VMEM((PANELS, COLS, WIDTH), F32),
            pltpu.VMEM((PANELS, 2, 3, COLS // 8, WIDTH), F32),
            pltpu.VMEM((PANELS, COLS, WIDTH), F32),
            pltpu.VMEM((WIDTH, WIDTH), BF16),
            pltpu.VMEM((WIDTH, WIDTH), BF16),
            dma((PANELS,)),
            dma,
            dma((2,)),
            dma((9,)),
            dma((3,)),
            dma((3,)),
            dma((PIECES, 3)),
            dma((2, 3)),
            dma((2,)),
            dma((2,)),
            dma((PANELS, QUARTERS, 2)),
            dma((PANELS, QUARTERS, 2)),
            dma((PANELS, QUARTERS, 2)),
            dma((PANELS, QUARTERS, 2)),
            dma((PANELS, QUARTERS)),
            dma((PANELS,)),
            dma((PANELS,)),
            dma((PANELS,)),
            dma((PANELS, 2, 3)),
            dma((PANELS,)),
            dma((PANELS, 2, 3)),
            dma((PANELS,)),
        ],
        compiler_params=pltpu.CompilerParams(
            collective_id=0, has_side_effects=True, vmem_limit_bytes=49 * 2**20
        ),
    )(eigvecs, jnp.swapaxes(v_panels, 1, 2), jnp.swapaxes(t_panels, 1, 2))
    return pl.pallas_call(
        last_update,
        out_shape=jax.ShapeDtypeStruct((ROWS, COLS), F32),
        grid=(ROWS // BAND,),
        in_specs=[pl.BlockSpec(memory_space=pltpu.VMEM)] * 5,
        out_specs=pl.BlockSpec((BAND, COLS), lambda i: (i, 0)),
        compiler_params=pltpu.CompilerParams(vmem_limit_bytes=8 * 2**20),
    )(*[pltpu.with_memory_space_constraint(one, pltpu.VMEM) for one in state])


def solution(mesh):
    in_specs = (P("row", "col"), P(None, "row", "col"), P(None, None, "col"))
    out_specs = P("row", "col")
    return jax.shard_map(local, mesh=mesh, in_specs=in_specs, out_specs=out_specs, check_vma=False)
```
